32 devices in a mesh: row: 8 (over y, x, core), col: 4 (over z).
Axes of the slice: x: 2, y: 2, z: 4, core: 2. Of those that a mesh axis runs over, the one named last changes fastest.
Arguments:
- vectors: bfloat16 [32, 1024, 512], P('col', 'row'), may hold values from -6 to 6
- right_factors: bfloat16 [32, 32, 1024, 128], P('row', 'col'), may hold values from -0.1875 to 0.1875
- left_factors: bfloat16 [32, 32, 1024, 128], P('row', 'col'), may hold values from -0.125 to 0.125
- tile_ranks: int32 [32, 32], P('row', 'col'), may hold values from 16 to 128
- owner_map: int32 [32], replicated, may hold values from 0 to 31, as said below
Outputs:
- applied: bfloat16 [32, 1024, 512], P('row', 'col')
The draws below stay inside these ranges and needn't reach their ends.
Inputs may be any that keep to these rules, and one draw needn't show every extreme that they name: owner_map is a permutation of 0 to 31; the 4 stored tile rows held by index i of row (stored rows i * 4 to i * 4 + 3) belong to 4 different indices of row of applied, i + c mod 8 for the same 4 offsets c at every i.
All inputs are finite; a program needn't handle non-finite values.
Results may differ from the reference program's by a relative error of at most 0.0066.
Values may be sent and summed in bfloat16 or wider, within the bound.
A program may use at most 128 MiB of HBM per device.

```python
import jax
import jax.numpy as jnp
from jax import lax

BLK = 1024
RMAX = 128
TRD = 4
NV = 512
NT = 32
MT = 32
N_ROW = 8


def shuffle(subkey):
    return jax.random.permutation(subkey, TRD)


def draw_owner_map(key, part):
    key_shift, key_dest, key_source = jax.random.split(jax.random.fold_in(key, 17), 3)
    offsets = jnp.arange(N_ROW, dtype=jnp.int32)
    ranking = jax.random.permutation(key_shift, N_ROW).astype(jnp.int32)
    priority = jnp.where(offsets == N_ROW // 2, -2, jnp.where(offsets == 1, -1, ranking))
    shifts = jnp.argsort(priority)[:TRD].astype(jnp.int32)
    dest_order = jax.vmap(shuffle)(jax.random.split(key_dest, N_ROW)).astype(jnp.int32)
    source_order = jax.vmap(shuffle)(jax.random.split(key_source, N_ROW)).astype(jnp.int32)
    source = jnp.arange(N_ROW, dtype=jnp.int32)[:, None]
    group_index = jnp.broadcast_to(jnp.arange(TRD, dtype=jnp.int32)[None, :], (N_ROW, TRD))
    target = (source + shifts[None, :]) % N_ROW
    landing = target * TRD + dest_order[target, group_index]
    places = source * TRD + source_order
    return jnp.zeros((MT,), jnp.int32).at[places.reshape(-1)].set(landing.reshape(-1))


def with_ends(entries, own_key, low, top_value):
    place = [jax.random.randint(jax.random.fold_in(own_key, axis), (), 0, length) for axis, length in enumerate(entries.shape)]
    main_axis = entries.shape.index(max(entries.shape))
    neighbour = place[:main_axis] + [(place[main_axis] + 1) % entries.shape[main_axis]] + place[main_axis + 1:]
    return entries.at[tuple(place)].set(low).at[tuple(neighbour)].set(top_value)


def block_scale(own_key, extent, cuts, least, largest):
    level, own = 1.0, jax.random.fold_in(own_key, 6)
    for axis_at, shards_of in cuts:
        heights = jnp.exp(jax.random.uniform(jax.random.fold_in(own, axis_at), (shards_of,), jnp.float32, least / len(cuts), largest / len(cuts)))
        level = level * jnp.repeat(heights, extent[axis_at] // shards_of).reshape([-1 if axis == axis_at else 1 for axis in range(len(extent))])
    return level


def centred(key, dims, width, limit, shards=(), kind=jnp.bfloat16):
    values = jax.random.normal(key, dims, jnp.float32) * width
    if len(shards) > 0:
        values = block_scale(key, dims, shards, -0.22, 0.18) * values
    return jnp.clip(values, min=-limit, max=limit).astype(kind)


def setup_inputs(seed: int = 0) -> dict:
    keys = jax.random.split(jax.random.key(seed), 6)
    return {
        "vectors": centred(keys[0], (NT, BLK, NV), 1.0, 6.0, ((0, 4), (1, 8))),
        "right_factors": centred(keys[1], (MT, NT, BLK, RMAX), BLK ** -0.5, 0.1875, ((0, 8), (1, 4))),
        "left_factors": centred(keys[2], (MT, NT, BLK, RMAX), (NT * RMAX // 2) ** -0.5, 0.125, ((0, 8), (1, 4))),
        "tile_ranks": with_ends(jax.random.randint(keys[3], (MT, NT), RMAX // 8, RMAX + 1), jax.random.fold_in(keys[3], 1), RMAX // 8, RMAX).astype(jnp.int32),
        "owner_map": draw_owner_map(jax.random.fold_in(keys[5], 71), 0),
    }


def reference(vectors, right_factors, left_factors, tile_ranks, owner_map):
    columns = jnp.arange(RMAX, dtype=jnp.int32)
    wide_vectors = vectors.astype(jnp.float32)

    def tile_row(operands):
        left_row, right_row, rank_row = operands
        products = jnp.einsum("kbr,kbv->krv", right_row.astype(jnp.float32), wide_vectors)
        kept_mask = columns[None, :] < rank_row[:, None]
        coeffs = jnp.where(kept_mask[:, :, None], products, 0.0).astype(jnp.bfloat16)
        return jnp.einsum("kbr,krv->bv", left_row.astype(jnp.float32), coeffs.astype(jnp.float32))

    stored = lax.map(tile_row, (left_factors, right_factors, tile_ranks))
    natural = jnp.zeros(stored.shape, jnp.float32).at[owner_map].set(stored)
    return natural.astype(jnp.bfloat16)
```

```python
import functools

import jax
import jax.numpy as jnp
from jax import lax
from jax.experimental import pallas as pl
from jax.experimental.pallas import tpu as pltpu
from jax.sharding import PartitionSpec as P

MESH = pl.DeviceIdType.MESH
LANES = 128
PIECES = 2


def kernel(n_row, n_col, n_chunk, owner_map, tile_ranks, vectors, right, left, out, *scratch):
    (gathered, right_raw, right_t, left_v, coeffs, own_part, z_send, z_recv, final, a_send) = scratch[:10]
    a_recv = scratch[10 : 10 + n_chunk]
    (load_sem, fac_sem, ag_ssem, ag_rsem, fw_ssem, fw_rsem, z_ssem, z_rsem, a_ssem, a_rsem) = scratch[
        10 + n_chunk :
    ]
    held, tiles, block, rank_width = right_raw.shape
    depth = vectors.shape[1]
    width = gathered.shape[3]
    quarter = out.shape[1]
    n_chip = n_row // 2
    per_piece = held // PIECES
    me = lax.axis_index("row")
    z = lax.axis_index("col")
    chip, core = me // 2, me % 2
    partner = me + 1 - 2 * core

    def own_load(v):
        return pltpu.make_async_copy(
            vectors.at[:, :, pl.ds(v * width, width)],
            gathered.at[v, :, pl.ds(pl.multiple_of(me * depth, depth), depth), :],
            load_sem.at[v],
        )

    for v in range(n_chunk):
        own_load(v).start()
    right_load = pltpu.make_async_copy(right, right_raw, fac_sem.at[0])
    left_load = pltpu.make_async_copy(left, left_v, fac_sem.at[1])
    right_load.start()
    left_load.start()

    barrier = pltpu.get_barrier_semaphore()
    for d in range(1, n_row):
        pl.semaphore_signal(barrier, inc=1, device_id=((me + d) % n_row, z), device_id_type=MESH)

    @pl.when(z > 0)
    def _():
        pl.semaphore_signal(barrier, inc=1, device_id=(me, z - 1), device_id_type=MESH)

    @pl.when(z < n_col - 1)
    def _():
        pl.semaphore_signal(barrier, inc=1, device_id=(me, z + 1), device_id_type=MESH)

    both = jnp.where(z > 0, 1, 0) + jnp.where(z < n_col - 1, 1, 0)
    pl.semaphore_wait(barrier, n_row - 1 + both)

    def rows_of(v, index):
        return gathered.at[v, :, pl.ds(pl.multiple_of(index * depth, depth), depth), :]

    def gather_copy(v, d, index):
        target = ((chip + d) % n_chip) * 2 + core
        return pltpu.make_async_remote_copy(
            src_ref=rows_of(v, index),
            dst_ref=rows_of(v, index),
            send_sem=ag_ssem.at[v, d - 1],
            recv_sem=ag_rsem.at[v, d - 1],
            device_id=(target, z),
            device_id_type=MESH,
        )

    def forward_copy(v, d, index):
        return pltpu.make_async_remote_copy(
            src_ref=rows_of(v, index),
            dst_ref=rows_of(v, index),
            send_sem=fw_ssem.at[v, d],
            recv_sem=fw_rsem.at[v, d],
            device_id=(partner, z),
            device_id_type=MESH,
        )

    def source(d, of_core):
        return ((chip + n_chip - d) % n_chip) * 2 + of_core

    def gather_start(v):
        own_load(v).wait()
        for d in range(1, n_chip):
            gather_copy(v, d, me).start()
        forward_copy(v, 0, me).start()

    def gather_forward(v):
        for d in range(1, n_chip):
            gather_copy(v, d, source(d, core)).wait_recv()
            forward_copy(v, d, source(d, core)).start()

    def gather_finish(v):
        for d in range(n_chip):
            forward_copy(v, d, source(d, 1 - core)).wait_recv()

    below, above = z, n_col - 1 - z
    skew = jnp.where(above > below, above - below, below - above)
    nearest = jnp.where(above > below, below, above)
    farthest = jnp.where(above > below, above, below)
    far_sign = jnp.where(above > below, 1, -1)

    def share_at(k):
        late = k - skew
        paired = z + (nearest - late // 2) * (1 - 2 * (late % 2))
        return jnp.where(k < skew, z + far_sign * (farthest - k), paired)

    def partial_rows(s, share):
        rows = pl.ds(pl.multiple_of(share * quarter, quarter), quarter)
        lhs = jnp.concatenate([left_v[s, j, rows, :] for j in range(tiles)], axis=1)
        return jnp.dot(
            lhs, coeffs[s].reshape(tiles * rank_width, width), preferred_element_type=jnp.float32
        )

    def z_copy(v, share, piece, upward, target):
        span = pl.ds(piece * per_piece, per_piece)
        return pltpu.make_async_remote_copy(
            src_ref=z_send.at[v, share, span],
            dst_ref=z_recv.at[upward, v, share, span],
            send_sem=z_ssem.at[v, share, piece],
            recv_sem=z_rsem.at[upward, v, share, piece],
            device_id=(me, target),
            device_id_type=MESH,
        )

    def project(v):
        def tile(j, _):
            products = jnp.dot(right_t[j], gathered[v, j], preferred_element_type=jnp.float32)
            ids = lax.broadcasted_iota(jnp.int32, (rank_width, width), 0)
            for s in range(held):
                part = products[s * rank_width : (s + 1) * rank_width]
                coeffs[s, j] = jnp.where(ids < tile_ranks[s, j], part, 0.0).astype(jnp.bfloat16)
            return 0

        lax.fori_loop(0, tiles, tile, 0)

    def send_shares(v):
        for k in range(n_col - 1):
            share = share_at(k)
            upward = jnp.where(share > z, 1, 0)
            target = z + 2 * upward - 1
            has_input = jnp.where(upward == 1, below, above) > 0
            for piece in range(PIECES):

                @pl.when(has_input)
                def _():
                    z_copy(v, share, piece, upward, target).wait_recv()

                    def row(s, _):
                        total = partial_rows(s, share) + z_recv[upward, v, share, s].astype(jnp.float32)
                        z_send[v, share, s] = total.astype(jnp.bfloat16)
                        return 0

                    lax.fori_loop(piece * per_piece, (piece + 1) * per_piece, row, 0)

                @pl.when(jnp.logical_not(has_input))
                def _():
                    def row(s, _):
                        z_send[v, share, s] = partial_rows(s, share).astype(jnp.bfloat16)
                        return 0

                    lax.fori_loop(piece * per_piece, (piece + 1) * per_piece, row, 0)

                z_copy(v, share, piece, upward, target).start()

    def own_share(v):
        def row(s, _):
            own_part[v, s] = partial_rows(s, z)
            return 0

        lax.fori_loop(0, held, row, 0)

    def exchange_copy(v, d):
        return pltpu.make_async_remote_copy(
            src_ref=a_send.at[v, d],
            dst_ref=a_recv[v].at[d],
            send_sem=a_ssem.at[v, d],
            recv_sem=a_rsem.at[v, d],
            device_id=((me + d) % n_row, z),
            device_id_type=MESH,
        )

    def finalize(v):
        for has_input, upward in ((below > 0, 1), (above > 0, 0)):

            @pl.when(has_input)
            def _():
                other = z + 1 - 2 * upward
                for piece in range(PIECES):
                    z_copy(v, z, piece, upward, other).wait_recv()

                def row(s, _):
                    own_part[v, s] = own_part[v, s] + z_recv[upward, v, z, s].astype(jnp.float32)
                    return 0

                lax.fori_loop(0, held, row, 0)

        for s in range(held):
            final[s] = own_part[v, s].astype(jnp.bfloat16)
        for d in range(n_row - 1, -1, -1):
            target = (me + d) % n_row
            slot = jnp.int32(0)
            for s in range(held):
                slot = jnp.where(owner_map[me * held + s] // held == target, s, slot)
            if d == 0:
                a_recv[v][0] = final[slot]
            else:
                a_send[v, d] = final[slot]
                exchange_copy(v, d).start()

    def write_rows(v):
        for d in range(1, n_row):
            exchange_copy(v, d).wait_recv()
        for k in range(held):
            wanted = me * held + k
            holder = jnp.int32(0)
            for s in range(n_row * held):
                holder = jnp.where(owner_map[s] == wanted, s // held, holder)
            shift = (me + n_row - holder) % n_row
            out[k, :, v * width : (v + 1) * width] = a_recv[v][shift]

    gather_start(0)
    if n_chunk > 1:
        gather_start(1)
    right_load.wait()

    def flip(j, _):
        for s in range(held):
            right_t[j, s * rank_width : (s + 1) * rank_width, :] = right_raw[s, j].T
        return 0

    lax.fori_loop(0, tiles, flip, 0)
    left_load.wait()
    gather_forward(0)
    for v in range(n_chunk):
        if v + 2 < n_chunk:
            gather_start(v + 2)
        gather_finish(v)
        project(v)
        send_shares(v)
        own_share(v)
        if v + 1 < n_chunk:
            gather_forward(v + 1)
        if v > 0:
            finalize(v - 1)
        if v > 1:
            write_rows(v - 2)
    finalize(n_chunk - 1)
    if n_chunk > 1:
        write_rows(n_chunk - 2)
    write_rows(n_chunk - 1)

    for v in range(n_chunk):
        for d in range(1, n_chip):
            gather_copy(v, d, me).wait_send()
        for d in range(n_chip):
            forward_copy(v, d, me).wait_send()
        for k in range(n_col - 1):
            for piece in range(PIECES):
                z_copy(v, share_at(k), piece, 0, z).wait_send()
        for d in range(1, n_row):
            exchange_copy(v, d).wait_send()


def on_device(n_row, n_col, vectors, right_factors, left_factors, tile_ranks, owner_map):
    held, tiles, block, rank_width = right_factors.shape
    width = LANES
    n_vec = vectors.shape[2]
    n_chunk = n_vec // width
    quarter = block // n_col
    n_chip = n_row // 2
    bf16, f32 = jnp.bfloat16, jnp.float32
    dma = pltpu.SemaphoreType.DMA
    smem = pl.BlockSpec(memory_space=pltpu.SMEM)
    hbm = pl.BlockSpec(memory_space=pl.ANY)
    return pl.pallas_call(
        functools.partial(kernel, n_row, n_col, n_chunk),
        out_shape=jax.ShapeDtypeStruct((held, quarter, n_vec), bf16),
        in_specs=[smem, smem, hbm, hbm, hbm],
        out_specs=pl.BlockSpec(memory_space=pltpu.VMEM),
        scratch_shapes=[
            pltpu.VMEM((n_chunk, tiles, block, width), bf16),
            pltpu.VMEM((held, tiles, block, rank_width), bf16),
            pltpu.VMEM((tiles, held * rank_width, block), bf16),
            pltpu.VMEM((held, tiles, block, rank_width), bf16),
            pltpu.VMEM((held, tiles, rank_width, width), bf16),
            pltpu.VMEM((n_chunk, held, quarter, width), f32),
            pltpu.VMEM((n_chunk, n_col, held, quarter, width), bf16),
            pltpu.VMEM((2, n_chunk, n_col, held, quarter, width), bf16),
            pltpu.VMEM((held, quarter, width), bf16),
            pltpu.VMEM((n_chunk, n_row, quarter, width), bf16),
        ]
        + [pltpu.VMEM((n_row, quarter, width), bf16) for _ in range(n_chunk)]
        + [
            dma((n_chunk,)),
            dma((2,)),
            dma((n_chunk, n_chip - 1)),
            dma((n_chunk, n_chip - 1)),
            dma((n_chunk, n_chip)),
            dma((n_chunk, n_chip)),
            dma((n_chunk, n_col, PIECES)),
            dma((2, n_chunk, n_col, PIECES)),
            dma((n_chunk, n_row)),
            dma((n_chunk, n_row)),
        ],
        compiler_params=pltpu.CompilerParams(
            collective_id=0, has_side_effects=True, vmem_limit_bytes=60 * 1024 * 1024
        ),
    )(owner_map, tile_ranks, vectors, right_factors, left_factors)


def solution(mesh):
    placed = (
        P("col", "row", None),
        P("row", "col", None, None),
        P("row", "col", None, None),
        P("row", "col"),
        P(),
    )
    body = functools.partial(on_device, mesh.shape["row"], mesh.shape["col"])
    return jax.shard_map(
        body, mesh=mesh, in_specs=placed, out_specs=P("row", "col", None), check_vma=False
    )
```

```python
import functools

import jax
import jax.numpy as jnp
from jax import lax
from jax.experimental import pallas as pl
from jax.experimental.pallas import tpu as pltpu
from jax.sharding import PartitionSpec as P

MESH = pl.DeviceIdType.MESH
LANES = 128
PIECES = 2
PARTS = 4


def kernel(n_row, n_col, n_chunk, owner_map, tile_ranks, vectors, right, left, out, *scratch):
    (gathered, right_raw, right_t, left_v, coeffs, share_part, own_part, z_send, z_recv, final) = scratch[:10]
    a_send = scratch[10]
    a_recv = scratch[11 : 11 + n_chunk]
    (load_sem, fac_sem, ag_ssem, ag_rsem, fw_ssem, fw_rsem, z_ssem, z_rsem, a_ssem, a_rsem) = scratch[
        11 + n_chunk :
    ]
    held, tiles, block, rank_width = right_raw.shape
    depth = vectors.shape[1]
    width = gathered.shape[3]
    quarter = out.shape[1]
    n_chip = n_row // 2
    per_piece = quarter // PIECES
    first_tiles = tiles // PARTS
    last = n_chunk - 1
    me = lax.axis_index("row")
    z = lax.axis_index("col")
    chip, core = me // 2, me % 2
    partner = me + 1 - 2 * core

    def own_load(v):
        return pltpu.make_async_copy(
            vectors.at[:, :, pl.ds(v * width, width)],
            gathered.at[v, :, pl.ds(pl.multiple_of(me * depth, depth), depth), :],
            load_sem.at[v],
        )

    for v in range(n_chunk):
        own_load(v).start()
    right_load = pltpu.make_async_copy(right, right_raw, fac_sem.at[0])
    left_load = pltpu.make_async_copy(left, left_v, fac_sem.at[1])
    right_load.start()
    left_load.start()

    barrier = pltpu.get_barrier_semaphore()
    for d in range(1, n_row):
        pl.semaphore_signal(barrier, inc=1, device_id=((me + d) % n_row, z), device_id_type=MESH)

    @pl.when(z > 0)
    def _():
        pl.semaphore_signal(barrier, inc=1, device_id=(me, z - 1), device_id_type=MESH)

    @pl.when(z < n_col - 1)
    def _():
        pl.semaphore_signal(barrier, inc=1, device_id=(me, z + 1), device_id_type=MESH)

    both = jnp.where(z > 0, 1, 0) + jnp.where(z < n_col - 1, 1, 0)
    pl.semaphore_wait(barrier, n_row - 1 + both)

    def parts_of(v):
        return PARTS if v == 0 else 1

    def slot_of(v, h):
        return h if v == 0 else PARTS - 1 + v

    def rows_of(v, h, index):
        span = pl.ds(h * first_tiles, first_tiles) if v == 0 else pl.ds(0, tiles)
        return gathered.at[v, span, pl.ds(pl.multiple_of(index * depth, depth), depth), :]

    def gather_copy(v, h, d, index):
        target = ((chip + d) % n_chip) * 2 + core
        return pltpu.make_async_remote_copy(
            src_ref=rows_of(v, h, index),
            dst_ref=rows_of(v, h, index),
            send_sem=ag_ssem.at[slot_of(v, h), d - 1],
            recv_sem=ag_rsem.at[slot_of(v, h), d - 1],
            device_id=(target, z),
            device_id_type=MESH,
        )

    def forward_copy(v, h, d, index):
        return pltpu.make_async_remote_copy(
            src_ref=rows_of(v, h, index),
            dst_ref=rows_of(v, h, index),
            send_sem=fw_ssem.at[slot_of(v, h), d],
            recv_sem=fw_rsem.at[slot_of(v, h), d],
            device_id=(partner, z),
            device_id_type=MESH,
        )

    def source(d, of_core):
        return ((chip + n_chip - d) % n_chip) * 2 + of_core

    def gather_start(v):
        own_load(v).wait()
        for h in range(parts_of(v)):
            for d in range(1, n_chip):
                gather_copy(v, h, d, me).start()
            forward_copy(v, h, 0, me).start()

    def gather_forward(v, h):
        for d in range(1, n_chip):
            gather_copy(v, h, d, source(d, core)).wait_recv()
            forward_copy(v, h, d, source(d, core)).start()

    def gather_finish(v, h):
        for d in range(n_chip):
            forward_copy(v, h, d, source(d, 1 - core)).wait_recv()

    below, above = z, n_col - 1 - z
    skew = jnp.where(above > below, above - below, below - above)
    nearest = jnp.where(above > below, below, above)
    farthest = jnp.where(above > below, above, below)
    far_sign = jnp.where(above > below, 1, -1)

    def share_at(k):
        late = k - skew
        paired = z + (nearest - late // 2) * far_sign * (2 * (late % 2) - 1)
        return jnp.where(k < skew, z + far_sign * (farthest - k), paired)

    def partial_rows(s, share):
        rows = pl.ds(pl.multiple_of(share * quarter, quarter), quarter)
        lhs = jnp.concatenate([left_v[s, j, rows, :] for j in range(tiles)], axis=1)
        return jnp.dot(
            lhs, coeffs[s].reshape(tiles * rank_width, width), preferred_element_type=jnp.float32
        )

    def z_copy(v, share, piece, upward, target):
        span = pl.ds(piece * per_piece, per_piece)
        return pltpu.make_async_remote_copy(
            src_ref=z_send.at[v, share, :, span, :],
            dst_ref=z_recv.at[upward, v, share, :, span, :],
            send_sem=z_ssem.at[v, share, piece],
            recv_sem=z_rsem.at[upward, v, share, piece],
            device_id=(me, target),
            device_id_type=MESH,
        )

    def project(v, first, count):
        def tile(j, _):
            products = jnp.dot(right_t[j], gathered[v, j], preferred_element_type=jnp.float32)
            ids = lax.broadcasted_iota(jnp.int32, (rank_width, width), 0)
            for s in range(held):
                part = products[s * rank_width : (s + 1) * rank_width]
                coeffs[s, j] = jnp.where(ids < tile_ranks[s, j], part, 0.0).astype(jnp.bfloat16)
            return 0

        lax.fori_loop(first, first + count, tile, 0)

    def send_shares(v):
        for k in range(n_col - 1):
            share = share_at(k)
            upward = jnp.where(share > z, 1, 0)
            target = z + 2 * upward - 1
            has_input = jnp.where(upward == 1, below, above) > 0

            def row(s, _):
                share_part[s] = partial_rows(s, share)
                return 0

            lax.fori_loop(0, held, row, 0)
            for piece in range(PIECES):
                span = slice(piece * per_piece, (piece + 1) * per_piece)

                @pl.when(has_input)
                def _():
                    z_copy(v, share, piece, upward, target).wait_recv()
                    for s in range(held):
                        total = share_part[s, span] + z_recv[upward, v, share, s, span].astype(jnp.float32)
                        z_send[v, share, s, span] = total.astype(jnp.bfloat16)

                @pl.when(jnp.logical_not(has_input))
                def _():
                    for s in range(held):
                        z_send[v, share, s, span] = share_part[s, span].astype(jnp.bfloat16)

                z_copy(v, share, piece, upward, target).start()

    def own_share(v):
        def row(s, _):
            own_part[v, s] = partial_rows(s, z)
            return 0

        lax.fori_loop(0, held, row, 0)

    def cuts_of(v):
        return PIECES if v == last else 1

    def exchange_copy(v, cut, d):
        size = quarter // cuts_of(v)
        span = pl.ds(cut * size, size)
        return pltpu.make_async_remote_copy(
            src_ref=a_send.at[v, d, span, :],
            dst_ref=a_recv[v].at[d, span, :],
            send_sem=a_ssem.at[v + cut, d],
            recv_sem=a_rsem.at[v + cut, d],
            device_id=((me + d) % n_row, z),
            device_id_type=MESH,
        )

    def finalize(v):
        slots = []
        for d in range(n_row):
            target = (me + d) % n_row
            slot = jnp.int32(0)
            for s in range(held):
                slot = jnp.where(owner_map[me * held + s] // held == target, s, slot)
            slots.append(slot)
        size = quarter // cuts_of(v)
        for cut in range(cuts_of(v)):
            span = slice(cut * size, (cut + 1) * size)
            for has_input, upward in ((below > 0, 1), (above > 0, 0)):

                @pl.when(has_input)
                def _():
                    other = z + 1 - 2 * upward
                    for piece in range(PIECES):
                        if piece * per_piece // size == cut:
                            z_copy(v, z, piece, upward, other).wait_recv()
                    for s in range(held):
                        own_part[v, s, span] = own_part[v, s, span] + z_recv[upward, v, z, s, span].astype(
                            jnp.float32
                        )

            for s in range(held):
                final[s, span] = own_part[v, s, span].astype(jnp.bfloat16)
            for d in range(n_row - 1, -1, -1):
                if d == 0:
                    a_recv[v][0, span] = final[slots[d], span]
                else:
                    a_send[v, d, span] = final[slots[d], span]
                    exchange_copy(v, cut, d).start()

    def write_rows(v):
        for cut in range(cuts_of(v)):
            for d in range(1, n_row):
                exchange_copy(v, cut, d).wait_recv()
        for k in range(held):
            wanted = me * held + k
            holder = jnp.int32(0)
            for s in range(n_row * held):
                holder = jnp.where(owner_map[s] == wanted, s // held, holder)
            shift = (me + n_row - holder) % n_row
            out[k, :, v * width : (v + 1) * width] = a_recv[v][shift]

    gather_start(0)
    right_load.wait()

    def flip(j, _):
        for s in range(held):
            right_t[j, s * rank_width : (s + 1) * rank_width, :] = right_raw[s, j].T
        return 0

    lax.fori_loop(0, tiles, flip, 0)
    left_load.wait()
    for v in range(n_chunk):
        if v == 0:
            for h in range(PARTS):
                gather_forward(0, h)
                if h == PARTS - 1 and n_chunk > 1:
                    gather_start(1)
                gather_finish(0, h)
                project(0, h * first_tiles, first_tiles)
        else:
            gather_finish(v, 0)
            project(v, 0, tiles)
        send_shares(v)
        own_share(v)
        if v + 1 < n_chunk:
            gather_forward(v + 1, 0)
        if v + 2 < n_chunk:
            gather_start(v + 2)
        if v > 0:
            finalize(v - 1)
        if v > 1:
            write_rows(v - 2)
    if n_chunk > 1:
        finalize(last)
        write_rows(last - 1)
    else:
        finalize(last)
    write_rows(last)

    for v in range(n_chunk):
        for h in range(parts_of(v)):
            for d in range(1, n_chip):
                gather_copy(v, h, d, me).wait_send()
            for d in range(n_chip):
                forward_copy(v, h, d, me).wait_send()
        for k in range(n_col - 1):
            for piece in range(PIECES):
                z_copy(v, share_at(k), piece, 0, z).wait_send()
        for cut in range(cuts_of(v)):
            for d in range(1, n_row):
                exchange_copy(v, cut, d).wait_send()


def on_device(n_row, n_col, vectors, right_factors, left_factors, tile_ranks, owner_map):
    held, tiles, block, rank_width = right_factors.shape
    width = LANES
    n_vec = vectors.shape[2]
    n_chunk = n_vec // width
    quarter = block // n_col
    n_chip = n_row // 2
    bf16, f32 = jnp.bfloat16, jnp.float32
    dma = pltpu.SemaphoreType.DMA
    smem = pl.BlockSpec(memory_space=pltpu.SMEM)
    hbm = pl.BlockSpec(memory_space=pl.ANY)
    return pl.pallas_call(
        functools.partial(kernel, n_row, n_col, n_chunk),
        out_shape=jax.ShapeDtypeStruct((held, quarter, n_vec), bf16),
        in_specs=[smem, smem, hbm, hbm, hbm],
        out_specs=pl.BlockSpec(memory_space=pltpu.VMEM),
        scratch_shapes=[
            pltpu.VMEM((n_chunk, tiles, block, width), bf16),
            pltpu.VMEM((held, tiles, block, rank_width), bf16),
            pltpu.VMEM((tiles, held * rank_width, block), bf16),
            pltpu.VMEM((held, tiles, block, rank_width), bf16),
            pltpu.VMEM((held, tiles, rank_width, width), bf16),
            pltpu.VMEM((held, quarter, width), f32),
            pltpu.VMEM((n_chunk, held, quarter, width), f32),
            pltpu.VMEM((n_chunk, n_col, held, quarter, width), bf16),
            pltpu.VMEM((2, n_chunk, n_col, held, quarter, width), bf16),
            pltpu.VMEM((held, quarter, width), bf16),
            pltpu.VMEM((n_chunk, n_row, quarter, width), bf16),
        ]
        + [pltpu.VMEM((n_row, quarter, width), bf16) for _ in range(n_chunk)]
        + [
            dma((n_chunk,)),
            dma((2,)),
            dma((n_chunk + PARTS - 1, n_chip - 1)),
            dma((n_chunk + PARTS - 1, n_chip - 1)),
            dma((n_chunk + PARTS - 1, n_chip)),
            dma((n_chunk + PARTS - 1, n_chip)),
            dma((n_chunk, n_col, PIECES)),
            dma((2, n_chunk, n_col, PIECES)),
            dma((n_chunk + PIECES - 1, n_row)),
            dma((n_chunk + PIECES - 1, n_row)),
        ],
        compiler_params=pltpu.CompilerParams(
            collective_id=0, has_side_effects=True, vmem_limit_bytes=60 * 1024 * 1024
        ),
    )(owner_map, tile_ranks, vectors, right_factors, left_factors)


def solution(mesh):
    placed = (
        P("col", "row", None),
        P("row", "col", None, None),
        P("row", "col", None, None),
        P("row", "col"),
        P(),
    )
    body = functools.partial(on_device, mesh.shape["row"], mesh.shape["col"])
    return jax.shard_map(
        body, mesh=mesh, in_specs=placed, out_specs=P("row", "col", None), check_vma=False
    )
```
